512 devices in a mesh: lat: 128 (over x, z_lo, y), chan: 4 (over z_hi, core).
Axes of the slice: x: 4, y: 8, z: 8 (z_hi: 2, z_lo: 4; z = z_hi * 4 + z_lo), core: 2. Of those that a mesh axis runs over, the one named last changes fastest.
Arguments:
- field: bfloat16 [640, 642, 544], P('lat', None, 'chan'), may hold values from -6 to 6
- cotangent: bfloat16 [640, 642, 1024], P('lat'), may hold values from -24 to 24
- weight: bfloat16 [544, 1024], P('chan'), may hold values from -0.25 to 0.25
- lon_counts: int32 [640], P('lat'), may hold values from 20 to 5136, as said below
- point_mask: int32 [640, 5136], P('lat', 'chan'), may hold values 0 or 1
Outputs:
- field_grad: bfloat16 [640, 642, 544], P('lat', None, 'chan')
- weight_grad: float32 [1024, 544], P('lat', 'chan')
The draws below stay inside these ranges and needn't reach their ends.
Inputs may be any that keep to these rules, and one draw needn't show every extreme that they name: `lon_counts`: number of longitudes in use in a row; points from there to the end of the row are padding.
All inputs are finite; a program needn't handle non-finite values. No bound on the sum of `point_mask` on one device may be relied on, other than what follows from the above.
Results may differ from the reference program's by a relative error of at most 0.001.
Values sent between devices are 32-bit elements; how exact they have to be, the bound alone decides.
A program may use at most 64 MiB of HBM per device.

```python
import jax
import jax.numpy as jnp
from jax import lax

E = 1024
P_SIZE = 8
LON = 5136
C = 68
PATCHES = 642
ROWS = 640


def draw_lon_counts(key, part):
    row_index = jnp.arange(ROWS, dtype=jnp.int32)
    spread = max(1280 // ROWS, 1)
    latitude = row_index * 1280 // ROWS + jax.random.randint(key, (ROWS,), 0, spread, dtype=jnp.int32)
    latitude = jnp.minimum(latitude, 1279)
    latitude = jnp.where(row_index == ROWS - 1, 1279, latitude)
    latitude = jnp.where(row_index == 0, 0, latitude)
    return (20 + (LON - 20) * latitude // 1279).astype(jnp.int32)


def plant(values, own_key, least, largest):
    dims = values.shape
    place = [jax.random.randint(jax.random.fold_in(own_key, axis), (), 0, dims[axis]) for axis in range(len(dims))]
    values = values.at[tuple(place)].set(least)
    longest = dims.index(max(dims))
    place[longest] = (place[longest] + 1) % dims[longest]
    return values.at[tuple(place)].set(largest)


def strengthened(array, own_key, source, target, shards_of, factor):
    owner, partner = [(jnp.arange(array.shape[axis_at]) // (array.shape[axis_at] // shards_of)).reshape([-1 if axis == axis_at else 1 for axis in range(array.ndim)]) for axis_at in (source, target)]
    chosen = jax.random.permutation(own_key, shards_of)[partner]
    strong = (owner == chosen) | (owner == (partner + shards_of // 2) % shards_of)
    return jnp.where(strong, factor * array, array)


def steps_of(key, shape, split, low, top_value):
    loudness, own = 1.0, jax.random.fold_in(key, 6)
    for dim, parts in split:
        steps = jnp.exp(jax.random.uniform(jax.random.fold_in(own, dim), (parts,), jnp.float32, low / len(split), top_value / len(split)))
        loudness = loudness * jnp.repeat(steps, shape[dim] // parts).reshape([-1 if axis == dim else 1 for axis in range(len(shape))])
    return loudness


def centred(own_key, dims, width, bound, split=(), held_as=jnp.bfloat16):
    entries = jax.random.normal(own_key, dims, jnp.float32) * width
    if len(split) > 0:
        entries = steps_of(own_key, dims, split, -0.22, 0.18) * entries
    return jnp.clip(entries, min=-bound, max=bound).astype(held_as)


def heavy_noise(stream_key, shape, deviation, most, cuts, heavy, kind=jnp.bfloat16):
    drawn = deviation * jax.random.normal(stream_key, shape, jnp.float32)
    if cuts:
        drawn = drawn * steps_of(stream_key, shape, cuts, -0.22, 0.18)
    return jnp.clip(strengthened(drawn, jax.random.fold_in(stream_key, 3), *heavy), -most, most).astype(kind)


def setup_inputs(seed: int = 0) -> dict:
    splits = jax.random.split(jax.random.key(seed), 6)
    return {
        "field": centred(splits[0], (ROWS, PATCHES, C * P_SIZE), 1.0, 6.0, ((0, 128), (2, 4))),
        "cotangent": heavy_noise(splits[1], (ROWS, PATCHES, E), 1.0, 24.0, ((0, 128),), (0, 2, 128, 5.5)),
        "weight": centred(splits[2], (C * P_SIZE, E), (C * P_SIZE) ** -0.5, 0.25, ((0, 4),)),
        "lon_counts": draw_lon_counts(jax.random.fold_in(splits[5], 71), 0),
        "point_mask": plant((jax.random.randint(splits[4], (ROWS, LON), 0, 4) < 3).astype(jnp.int32), jax.random.fold_in(splits[4], 1), 0, 1),
    }


def reference(field, cotangent, weight, lon_counts, point_mask):
    positions = lax.broadcasted_iota(jnp.int32, point_mask.shape, 1)
    valid = jnp.where(positions < lon_counts[:, None], point_mask, 0)
    total = jnp.sum(valid).astype(jnp.float32)
    scale = lax.rsqrt(jnp.maximum(total, 1.0))
    point_valid = valid.reshape(ROWS, PATCHES, 1, P_SIZE)
    masked = (field.reshape(ROWS, PATCHES, C, P_SIZE) * point_valid.astype(jnp.bfloat16)).reshape(ROWS * PATCHES, C * P_SIZE)
    grads = cotangent.reshape(ROWS * PATCHES, E)
    product = lax.dot_general(grads, weight, (((1,), (1,)), ((), ())), preferred_element_type=jnp.float32)
    field_grad = (product.reshape(ROWS, PATCHES, C, P_SIZE) * point_valid.astype(jnp.float32)).reshape(ROWS, PATCHES, C * P_SIZE).astype(jnp.bfloat16)
    weight_grad = lax.dot_general(grads, masked, (((0,), (0,)), ((), ())), preferred_element_type=jnp.float32) * scale
    return (field_grad, weight_grad)
```

```python
import functools

import jax
import jax.numpy as jnp
from jax import lax
from jax.experimental import pallas as pl
from jax.experimental.pallas import tpu as pltpu
from jax.sharding import Mesh
from jax.sharding import PartitionSpec as P

MESH = pl.DeviceIdType.MESH
AXES = ("x", "z", "y", "zh", "core")
LAT = ("x", "z", "y")
CHAN = ("zh", "core")
F32 = jnp.float32
BF16 = jnp.bfloat16

ROWS = 5
PATCHES = 642
F = 136
E = 1024
PART = 1284
BASES = (0, 128, 256, 384)
WIDTHS = (256, 256, 256, 384)
LANES = 768
Z_ROWS = 72


def iota(shape, dim):
    return lax.broadcasted_iota(jnp.int32, shape, dim)


def kernel(
    ft_hbm, cot_hbm, w_hbm, counts, mask_hbm,
    fg_hbm, wg_ref,
    ft, cot, w, masks, pick, valid, prod, fm,
    x_send, x_recv, z_send, z_recv, y_send, y_recv,
    cot_sem, ft_sem, w_sem, mask_sem, out_sem,
    m_ssem, m_rsem, x_ssem, x_rsem, z_ssem, z_rsem, y_ssem, y_rsem,
):
    x, z, y = (lax.axis_index(a) for a in LAT)
    zh, core = (lax.axis_index(a) for a in CHAN)
    me = zh * 2 + core

    barrier = pltpu.get_barrier_semaphore()

    def greet(device):
        pl.semaphore_signal(barrier, inc=1, device_id=device, device_id_type=MESH)

    for d in range(1, 4):
        greet({"zh": zh ^ (d // 2), "core": core ^ (d % 2)})
    for d in range(1, 4):
        greet({"x": (x + d) % 4})
    for d in range(1, 4):
        greet({"z": (z + d) % 4})
    for d in range(1, 8):
        greet({"y": (y + d) % 8})

    own_mask = pltpu.make_async_copy(mask_hbm, masks.at[me], mask_sem)
    own_mask.start()
    w_copy = pltpu.make_async_copy(w_hbm, w, w_sem)
    w_copy.start()
    cot_copies = [pltpu.make_async_copy(cot_hbm.at[r], cot.at[r], cot_sem.at[r]) for r in range(ROWS)]
    ft_copies = [pltpu.make_async_copy(ft_hbm.at[r], ft.at[r], ft_sem.at[r]) for r in range(ROWS)]
    for c in cot_copies + ft_copies:
        c.start()

    own_mask.wait()
    pl.semaphore_wait(barrier, 16)

    mask_copies = []
    for d in (3, 2, 1):
        copy = pltpu.make_async_remote_copy(
            src_ref=masks.at[me],
            dst_ref=masks.at[me],
            send_sem=m_ssem.at[d - 1],
            recv_sem=m_rsem.at[d - 1],
            device_id={"zh": zh ^ (d // 2), "core": core ^ (d % 2)},
            device_id_type=MESH,
        )
        copy.start()
        mask_copies.append(copy)

    for j in range(4):
        at = (iota((PART, WIDTHS[j]), 0) + PART * j) // 8 - BASES[j]
        hit = at == iota((PART, WIDTHS[j]), 1)
        pick[j, :, : WIDTHS[j]] = jnp.where(hit, 1.0, 0.0).astype(BF16)
    valid[...] = jnp.zeros_like(valid)

    w_copy.wait()
    for r in range(ROWS):
        cot_copies[r].wait()
        for p in range(0, PATCHES, 256):
            n = min(256, PATCHES - p)
            prod[r, :, p : p + n] = lax.dot_general(
                w[...], cot[r, p : p + n, :], (((1,), (1,)), ((), ())), preferred_element_type=F32
            ).astype(BF16)

    for copy in mask_copies:
        copy.wait_recv()
    for c in ft_copies:
        c.wait()

    for j in range(4):
        spot = iota((8, PART), 1) + PART * j
        phase = spot % 8 == iota((8, PART), 0)
        rows = []
        for r in range(ROWS):
            keep = jnp.logical_and(phase, spot < counts[r])
            line = jnp.broadcast_to(masks[j, r : r + 1, :], (8, PART)).astype(F32)
            rows.append(jnp.where(keep, line, 0.0))
        spread = jnp.concatenate(rows, axis=0).astype(BF16)
        placed = jnp.dot(spread, pick[j, :, : WIDTHS[j]], preferred_element_type=F32)
        for r in range(ROWS):
            valid[r, :, BASES[j] : BASES[j] + WIDTHS[j]] += placed[8 * r : 8 * r + 8]

    count = jnp.zeros((8, 128), F32)
    for r in range(ROWS):
        v = valid[r]
        for t in range(LANES // 128):
            count = count + v[:, 128 * t : 128 * t + 128]
        v = v[:, :PATCHES]
        v16 = jnp.concatenate([v, v], axis=0).astype(BF16)
        for c in range(0, 128, 16):
            fm[r, c : c + 16, :] = ft[r, c : c + 16, :] * v16
        fm[r, 128:136, :] = ft[r, 128:136, :] * v16[:8]

    x_copies = []
    for d in (2, 1, 3, 0):
        to = (x + d) % 4
        lanes = pl.ds(pl.multiple_of(to * 256, 256), 256)
        acc = jnp.dot(fm[0], cot[0, :, lanes], preferred_element_type=F32)
        for r in range(1, ROWS):
            acc = acc + jnp.dot(fm[r], cot[r, :, lanes], preferred_element_type=F32)
        x_send[d, :F, :] = acc
        x_send[d, F : F + 8, :128] = count
        x_send[d, F : F + 8, 128:] = count
        if d:
            copy = pltpu.make_async_remote_copy(
                src_ref=x_send.at[d],
                dst_ref=x_recv.at[d - 1],
                send_sem=x_ssem.at[d - 1],
                recv_sem=x_rsem.at[d - 1],
                device_id={"x": to},
                device_id_type=MESH,
            )
            copy.start()
            x_copies.append(copy)

    out_copies = []
    for r in range(ROWS):
        v = valid[r][:, :PATCHES]
        v16 = jnp.concatenate([v, v], axis=0).astype(BF16)
        for c in range(0, 128, 16):
            prod[r, c : c + 16, :] = prod[r, c : c + 16, :] * v16
        prod[r, 128:136, :] = prod[r, 128:136, :] * v16[:8]
        copy = pltpu.make_async_copy(prod.at[r], fg_hbm.at[r], out_sem.at[r])
        copy.start()
        out_copies.append(copy)

    for copy in x_copies:
        copy.wait_recv()
    total = x_send[0] + x_recv[0] + x_recv[1] + x_recv[2]
    turned = jnp.transpose(total[:128, :])
    rest = total[128:F, :]
    counted = total[F : F + 8, :128] + pltpu.roll(total[F : F + 8, :128], 64, 1)
    half = iota((8, 128), 1) // 64
    for to in range(4):
        z_send[to, :64, :] = turned[64 * to : 64 * to + 64, :]
        tile = rest[:, 128 * (to // 2) : 128 * (to // 2) + 128]
        z_send[to, 64:72, :] = jnp.where(half == to % 2, tile, counted)

    z_copies = []
    for d in (2, 1, 3):
        to = (z + d) % 4
        copy = pltpu.make_async_remote_copy(
            src_ref=z_send.at[to],
            dst_ref=z_recv.at[d - 1],
            send_sem=z_ssem.at[d - 1],
            recv_sem=z_rsem.at[d - 1],
            device_id={"z": to},
            device_id_type=MESH,
        )
        copy.start()
        z_copies.append(copy)
    for copy in z_copies:
        copy.wait_recv()
    nearer = z_send[z] + z_recv[0] + z_recv[1] + z_recv[2]
    for to in range(8):
        y_send[to, :8, :] = nearer[8 * to : 8 * to + 8, :]
        y_send[to, 8:16, :] = nearer[64:72, :]

    y_copies = []
    for d in (4, 3, 5, 2, 6, 1, 7):
        to = (y + d) % 8
        copy = pltpu.make_async_remote_copy(
            src_ref=y_send.at[to],
            dst_ref=y_recv.at[d - 1],
            send_sem=y_ssem.at[d - 1],
            recv_sem=y_rsem.at[d - 1],
            device_id={"y": to},
            device_id_type=MESH,
        )
        copy.start()
        y_copies.append(copy)
    for copy in y_copies:
        copy.wait_recv()
    last = y_send[y]
    for d in range(7):
        last = last + y_recv[d]
    tile = last[8:16, :]
    other = jnp.where(half == z % 2, 0.0, tile)
    points = jnp.sum(jnp.sum(other, axis=1, keepdims=True), axis=0, keepdims=True)
    scale = lax.rsqrt(jnp.maximum(points, 1.0))
    wg_ref[:, :128] = last[:8, :] * scale
    moved = pltpu.roll(tile, (128 - ((z % 2) * 64 + y * 8)) % 128, 1)
    wg_ref[:, 128:136] = jnp.transpose(moved)[:8, :] * scale

    for copy in mask_copies + x_copies + z_copies + y_copies:
        copy.wait_send()
    for copy in out_copies:
        copy.wait()


def local(field, cotangent, weight, lon_counts, point_mask):
    ft = jnp.transpose(field, (0, 2, 1))
    any_space = pl.BlockSpec(memory_space=pl.ANY)
    dma = pltpu.SemaphoreType.DMA
    fg, wg = pl.pallas_call(
        kernel,
        out_shape=(
            jax.ShapeDtypeStruct((ROWS, F, PATCHES), BF16),
            jax.ShapeDtypeStruct((8, F), F32),
        ),
        in_specs=[any_space, any_space, any_space, pl.BlockSpec(memory_space=pltpu.SMEM), any_space],
        out_specs=(any_space, pl.BlockSpec(memory_space=pltpu.VMEM)),
        scratch_shapes=[
            pltpu.VMEM((ROWS, F, PATCHES), BF16),
            pltpu.VMEM((ROWS, PATCHES, E), BF16),
            pltpu.VMEM((F, E), BF16),
            pltpu.VMEM((4, ROWS, PART), jnp.int32),
            pltpu.VMEM((4, PART, 384), BF16),
            pltpu.VMEM((ROWS, 8, LANES), F32),
            pltpu.VMEM((ROWS, F, PATCHES), BF16),
            pltpu.VMEM((ROWS, F, PATCHES), BF16),
            pltpu.VMEM((4, F + 8, 256), F32),
            pltpu.VMEM((3, F + 8, 256), F32),
            pltpu.VMEM((4, Z_ROWS, 128), F32),
            pltpu.VMEM((3, Z_ROWS, 128), F32),
            pltpu.VMEM((8, 16, 128), F32),
            pltpu.VMEM((7, 16, 128), F32),
            dma((ROWS,)), dma((ROWS,)), dma, dma, dma((ROWS,)),
            dma((3,)), dma((3,)), dma((3,)), dma((3,)), dma((3,)), dma((3,)), dma((7,)), dma((7,)),
        ],
        compiler_params=pltpu.CompilerParams(
            collective_id=0, has_side_effects=True, vmem_limit_bytes=60 * 1024 * 1024
        ),
        name="backward",
    )(ft, cotangent, weight, lon_counts, point_mask)
    return jnp.transpose(fg, (0, 2, 1)), wg


def solution(mesh):
    split = Mesh(mesh.devices.reshape(4, 4, 8, 2, 2), AXES)
    in_specs = (P(LAT, None, CHAN), P(LAT, None, None), P(CHAN, None), P(LAT), P(LAT, CHAN))
    out_specs = (P(LAT, None, CHAN), P(LAT, CHAN))
    return jax.shard_map(local, mesh=split, in_specs=in_specs, out_specs=out_specs, check_vma=False)
```

```python
import functools

import jax
import jax.numpy as jnp
from jax import lax
from jax.experimental import pallas as pl
from jax.experimental.pallas import tpu as pltpu
from jax.sharding import Mesh
from jax.sharding import PartitionSpec as P

MESH = pl.DeviceIdType.MESH
AXES = ("x", "z", "y", "zh", "core")
LAT = ("x", "z", "y")
CHAN = ("zh", "core")
F32 = jnp.float32
BF16 = jnp.bfloat16

ROWS = 5
PATCHES = 642
F = 136
E = 1024
PART = 1284
WIDTH = 384
LANES = 768
Z_ROWS = 72


def iota(shape, dim):
    return lax.broadcasted_iota(jnp.int32, shape, dim)


def kernel(
    ft_hbm, cot_hbm, w_hbm, counts_hbm, mask_hbm,
    fg_ref, wg_ref,
    ft, cot, w, counts, masks, pick, valid, fm,
    x_send, x_recv, c_send, c_recv, z_send, z_recv, y_send, y_recv,
    cot_sem, ft_sem, w_sem, counts_sem, mask_sem,
    m_ssem, m_rsem, x_ssem, x_rsem, c_ssem, c_rsem, z_ssem, z_rsem, y_ssem, y_rsem,
):
    x, z, y = (lax.axis_index(a) for a in LAT)
    zh, core = (lax.axis_index(a) for a in CHAN)
    me = zh * 2 + core
    mate = zh * 2 + 1 - core
    far = (1 - zh) * 2 + core
    far_mate = (1 - zh) * 2 + 1 - core

    own_mask = pltpu.make_async_copy(mask_hbm, masks.at[me], mask_sem)
    own_mask.start()
    own_counts = pltpu.make_async_copy(counts_hbm, counts, counts_sem)
    own_counts.start()

    barrier = pltpu.get_barrier_semaphore()

    def greet(device):
        pl.semaphore_signal(barrier, inc=1, device_id=device, device_id_type=MESH)

    greet({"zh": 1 - zh})
    greet({"core": 1 - core})
    for d in (1, 2, 3):
        greet({"x": (x + d) % 4})
        greet({"z": (z + d) % 4})
    for d in range(1, 8):
        greet({"y": (y + d) % 8})

    shards = (me, mate, far, far_mate)
    for i, j in enumerate(shards):
        at = ((iota((PART, WIDTH), 0) + PART * j) >> 3) - 128 * j
        hit = at == iota((PART, WIDTH), 1)
        pick[i] = jnp.where(hit, 1.0, 0.0).astype(BF16)
    valid[...] = jnp.zeros_like(valid)

    own_mask.wait()
    own_counts.wait()
    w_copy = pltpu.make_async_copy(w_hbm, w, w_sem)
    cot_copies = [pltpu.make_async_copy(cot_hbm.at[r], cot.at[r], cot_sem.at[r]) for r in range(ROWS)]
    ft_copies = [pltpu.make_async_copy(ft_hbm.at[r], ft.at[r], ft_sem.at[r]) for r in range(ROWS)]

    def mask_to(i, shard, device):
        return pltpu.make_async_remote_copy(
            src_ref=masks.at[shard],
            dst_ref=masks.at[shard],
            send_sem=m_ssem.at[i],
            recv_sem=m_rsem.at[i],
            device_id=device,
            device_id_type=MESH,
        )

    def place(i):
        j = shards[i]
        spot = iota((8, PART), 1) + PART * j
        phase = (spot & 7) == iota((8, PART), 0)
        rows = []
        for r in range(ROWS):
            keep = jnp.logical_and(phase, spot < counts[r])
            line = jnp.broadcast_to(masks[j, r : r + 1, :], (8, PART)).astype(F32)
            rows.append(jnp.where(keep, line, 0.0))
        spread = jnp.concatenate(rows, axis=0).astype(BF16)
        placed = jnp.dot(spread, pick[i], preferred_element_type=F32)
        lanes = pl.ds(pl.multiple_of(j * 128, 128), WIDTH)
        for r in range(ROWS):
            valid[r, :, lanes] += placed[8 * r : 8 * r + 8]

    for c in ft_copies + cot_copies + [w_copy]:
        c.start()
    pl.semaphore_wait(barrier, 15)
    to_far = mask_to(0, me, {"zh": 1 - zh})
    to_far.start()
    to_mate = mask_to(1, me, {"core": 1 - core})
    to_mate.start()
    place(0)
    to_mate.wait_recv()
    place(1)
    to_far.wait_recv()
    relay = mask_to(2, far, {"core": 1 - core})
    relay.start()
    place(2)
    for c in ft_copies:
        c.wait()
    relay.wait_recv()
    place(3)

    count = jnp.zeros((8, 128), F32)
    for r in range(ROWS):
        v = valid[r]
        for t in range(LANES // 128):
            count = count + v[:, 128 * t : 128 * t + 128]
        v = v[:, :PATCHES]
        v16 = jnp.concatenate([v, v], axis=0).astype(BF16)
        for c in range(0, 128, 16):
            fm[r, c : c + 16, :] = ft[r, c : c + 16, :] * v16
        fm[r, 128:136, :] = ft[r, 128:136, :] * v16[:8]
    c_send[...] = count
    for c in cot_copies:
        c.wait()

    x_copies = []
    for d in (2, 1, 3, 0):
        to = (x + d) % 4
        lanes = pl.ds(pl.multiple_of(to * 256, 256), 256)
        acc = jnp.dot(fm[0], cot[0, :, lanes], preferred_element_type=F32)
        for r in range(1, ROWS):
            acc = acc + jnp.dot(fm[r], cot[r, :, lanes], preferred_element_type=F32)
        x_send[d] = acc
        if d:
            for source, target, ssem, rsem in (
                (x_send.at[d], x_recv.at[d - 1], x_ssem, x_rsem),
                (c_send, c_recv.at[d - 1], c_ssem, c_rsem),
            ):
                copy = pltpu.make_async_remote_copy(
                    src_ref=source,
                    dst_ref=target,
                    send_sem=ssem.at[d - 1],
                    recv_sem=rsem.at[d - 1],
                    device_id={"x": to},
                    device_id_type=MESH,
                )
                copy.start()
                x_copies.append(copy)

    w_copy.wait()
    for r in range(ROWS):
        v = valid[r][:, :PATCHES]
        v16 = jnp.concatenate([v] * 17, axis=0)
        for p in range(0, PATCHES, 256):
            n = min(256, PATCHES - p)
            product = lax.dot_general(
                w[...], cot[r, p : p + n, :], (((1,), (1,)), ((), ())), preferred_element_type=F32
            )
            fg_ref[r, :, p : p + n] = (product * v16[:, p : p + n]).astype(BF16)

    for copy in x_copies:
        copy.wait_recv()
    total = x_send[0] + x_recv[0] + x_recv[1] + x_recv[2]
    turned = jnp.transpose(total[:128, :])
    rest = total[128:F, :]
    counted = c_send[...] + c_recv[0] + c_recv[1] + c_recv[2]
    counted = counted + pltpu.roll(counted, 64, 1)
    half = iota((8, 128), 1) // 64
    for to in range(4):
        z_send[to, :64, :] = turned[64 * to : 64 * to + 64, :]
        tile = rest[:, 128 * (to // 2) : 128 * (to // 2) + 128]
        z_send[to, 64:72, :] = jnp.where(half == to % 2, tile, counted)

    z_copies = []
    for d in (2, 1, 3):
        to = (z + d) % 4
        copy = pltpu.make_async_remote_copy(
            src_ref=z_send.at[to],
            dst_ref=z_recv.at[d - 1],
            send_sem=z_ssem.at[d - 1],
            recv_sem=z_rsem.at[d - 1],
            device_id={"z": to},
            device_id_type=MESH,
        )
        copy.start()
        z_copies.append(copy)
    for copy in z_copies:
        copy.wait_recv()
    nearer = z_send[z] + z_recv[0] + z_recv[1] + z_recv[2]
    for to in range(8):
        y_send[to, :8, :] = nearer[8 * to : 8 * to + 8, :]
        y_send[to, 8:16, :] = nearer[64:72, :]

    y_copies = []
    for d in (4, 3, 5, 2, 6, 1, 7):
        to = (y + d) % 8
        copy = pltpu.make_async_remote_copy(
            src_ref=y_send.at[to],
            dst_ref=y_recv.at[d - 1],
            send_sem=y_ssem.at[d - 1],
            recv_sem=y_rsem.at[d - 1],
            device_id={"y": to},
            device_id_type=MESH,
        )
        copy.start()
        y_copies.append(copy)
    for copy in y_copies:
        copy.wait_recv()
    last = y_send[y]
    for d in range(7):
        last = last + y_recv[d]
    tile = last[8:16, :]
    other = jnp.where(half == z % 2, 0.0, tile)
    points = jnp.sum(jnp.sum(other, axis=1, keepdims=True), axis=0, keepdims=True)
    scale = lax.rsqrt(jnp.maximum(points, 1.0))
    wg_ref[:, :128] = last[:8, :] * scale
    moved = pltpu.roll(tile, (128 - ((z % 2) * 64 + y * 8)) % 128, 1)
    wg_ref[:, 128:136] = jnp.transpose(moved)[:8, :] * scale

    for copy in [to_far, to_mate, relay] + x_copies + z_copies + y_copies:
        copy.wait_send()


def local(field, cotangent, weight, lon_counts, point_mask):
    ft = jnp.transpose(field, (0, 2, 1))
    hbm = pl.BlockSpec(memory_space=pltpu.HBM)
    vmem = pl.BlockSpec(memory_space=pltpu.VMEM)
    dma = pltpu.SemaphoreType.DMA
    fg, wg = pl.pallas_call(
        kernel,
        out_shape=(pltpu.VMEM((ROWS, F, PATCHES), BF16), pltpu.VMEM((8, F), F32)),
        in_specs=[hbm] * 5,
        out_specs=(vmem, vmem),
        scratch_shapes=[
            pltpu.VMEM((ROWS, F, PATCHES), BF16),
            pltpu.VMEM((ROWS, PATCHES, E), BF16),
            pltpu.VMEM((F, E), BF16),
            pltpu.SMEM((ROWS,), jnp.int32),
            pltpu.VMEM((4, ROWS, PART), jnp.int32),
            pltpu.VMEM((4, PART, WIDTH), BF16),
            pltpu.VMEM((ROWS, 8, LANES), F32),
            pltpu.VMEM((ROWS, F, PATCHES), BF16),
            pltpu.VMEM((4, F, 256), F32),
            pltpu.VMEM((3, F, 256), F32),
            pltpu.VMEM((8, 128), F32),
            pltpu.VMEM((3, 8, 128), F32),
            pltpu.VMEM((4, Z_ROWS, 128), F32),
            pltpu.VMEM((3, Z_ROWS, 128), F32),
            pltpu.VMEM((8, 16, 128), F32),
            pltpu.VMEM((7, 16, 128), F32),
            dma((ROWS,)), dma((ROWS,)), dma, dma, dma,
            dma((3,)), dma((3,)), dma((3,)), dma((3,)), dma((3,)), dma((3,)),
            dma((3,)), dma((3,)), dma((7,)), dma((7,)),
        ],
        compiler_params=pltpu.CompilerParams(
            collective_id=0, has_side_effects=True, vmem_limit_bytes=40 * 1024 * 1024
        ),
        name="backward",
    )(*(pltpu.with_memory_space_constraint(v, pltpu.HBM) for v in (ft, cotangent, weight, lon_counts, point_mask)))
    return jnp.transpose(fg, (0, 2, 1)), wg


def solution(mesh):
    split = Mesh(mesh.devices.reshape(4, 4, 8, 2, 2), AXES)
    in_specs = (P(LAT, None, CHAN), P(LAT, None, None), P(CHAN, None), P(LAT), P(LAT, CHAN))
    out_specs = (P(LAT, None, CHAN), P(LAT, CHAN))
    return jax.shard_map(local, mesh=split, in_specs=in_specs, out_specs=out_specs, check_vma=False)
```

```python
import functools

import jax
import jax.numpy as jnp
from jax import lax
from jax.experimental import pallas as pl
from jax.experimental.pallas import tpu as pltpu
from jax.sharding import Mesh
from jax.sharding import PartitionSpec as P

MESH = pl.DeviceIdType.MESH
AXES = ("x", "z", "y", "zh", "core")
LAT = ("x", "z", "y")
CHAN = ("zh", "core")
F32 = jnp.float32
BF16 = jnp.bfloat16

ROWS = 5
PATCHES = 642
F = 136
E = 1024
PART = 1284
WIDTH = 384
LANES = 768
Z_ROWS = 72
TOP = 72


def iota(shape, dim):
    return lax.broadcasted_iota(jnp.int32, shape, dim)


def kernel(
    ft_hbm, cot_hbm, w_hbm, counts_hbm, mask_hbm,
    fg_ref, wg_ref,
    ft, cot, w, counts, masks, pick, valid, fm,
    x_two, x_up, x_down, x_own, s_up, s_down, r_up, r_down, c_send, c_recv, z_send, z_recv, y_send, y_recv,
    cot_sem, ft_sem, w_sem, counts_sem, mask_sem,
    m_ssem, m_rsem, u_ssem, u_rsem, d_ssem, d_rsem, c_ssem, c_rsem, z_ssem, z_rsem, y_ssem, y_rsem,
):
    x, z, y = (lax.axis_index(a) for a in LAT)
    zh, core = (lax.axis_index(a) for a in CHAN)
    me = zh * 2 + core
    mate = zh * 2 + 1 - core
    far = (1 - zh) * 2 + core
    far_mate = (1 - zh) * 2 + 1 - core

    own_mask = pltpu.make_async_copy(mask_hbm, masks.at[me], mask_sem)
    own_mask.start()
    own_counts = pltpu.make_async_copy(counts_hbm, counts, counts_sem)
    own_counts.start()

    barrier = pltpu.get_barrier_semaphore()

    def greet(device):
        pl.semaphore_signal(barrier, inc=1, device_id=device, device_id_type=MESH)

    greet({"zh": 1 - zh})
    greet({"core": 1 - core})
    for d in (1, 2, 3):
        greet({"x": (x + d) % 4})
        greet({"z": (z + d) % 4})
    for d in range(1, 8):
        greet({"y": (y + d) % 8})

    shards = (me, mate, far, far_mate)
    for i, j in enumerate(shards):
        at = ((iota((PART, WIDTH), 0) + PART * j) >> 3) - 128 * j
        hit = at == iota((PART, WIDTH), 1)
        pick[i] = jnp.where(hit, 1.0, 0.0).astype(BF16)
    valid[...] = jnp.zeros_like(valid)

    own_mask.wait()
    own_counts.wait()
    w_copy = pltpu.make_async_copy(w_hbm, w, w_sem)
    cot_copies = [pltpu.make_async_copy(cot_hbm.at[r], cot.at[r], cot_sem.at[r]) for r in range(ROWS)]
    ft_copies = [pltpu.make_async_copy(ft_hbm.at[r], ft.at[r], ft_sem.at[r]) for r in range(ROWS)]

    def mask_to(i, shard, device):
        return pltpu.make_async_remote_copy(
            src_ref=masks.at[shard],
            dst_ref=masks.at[shard],
            send_sem=m_ssem.at[i],
            recv_sem=m_rsem.at[i],
            device_id=device,
            device_id_type=MESH,
        )

    def place(i):
        j = shards[i]
        spot = iota((8, PART), 1) + PART * j
        phase = (spot & 7) == iota((8, PART), 0)
        rows = []
        for r in range(ROWS):
            keep = jnp.logical_and(phase, spot < counts[r])
            line = jnp.broadcast_to(masks[j, r : r + 1, :], (8, PART)).astype(F32)
            rows.append(jnp.where(keep, line, 0.0))
        spread = jnp.concatenate(rows, axis=0).astype(BF16)
        placed = jnp.dot(spread, pick[i], preferred_element_type=F32)
        lanes = pl.ds(pl.multiple_of(j * 128, 128), WIDTH)
        for r in range(ROWS):
            valid[r, :, lanes] += placed[8 * r : 8 * r + 8]

    for c in ft_copies + cot_copies + [w_copy]:
        c.start()
    pl.semaphore_wait(barrier, 15)
    to_far = mask_to(0, me, {"zh": 1 - zh})
    to_far.start()
    to_mate = mask_to(1, me, {"core": 1 - core})
    to_mate.start()
    place(0)
    to_mate.wait_recv()
    place(1)
    to_far.wait_recv()
    relay = mask_to(2, far, {"core": 1 - core})
    relay.start()
    place(2)
    for c in ft_copies:
        c.wait()
    relay.wait_recv()
    place(3)

    count = jnp.zeros((8, 128), F32)
    for r in range(ROWS):
        v = valid[r]
        for t in range(LANES // 128):
            count = count + v[:, 128 * t : 128 * t + 128]
        v = v[:, :PATCHES]
        v16 = jnp.concatenate([v, v], axis=0).astype(BF16)
        for c in range(0, 128, 16):
            fm[r, c : c + 16, :] = ft[r, c : c + 16, :] * v16
        fm[r, 128:136, :] = ft[r, 128:136, :] * v16[:8]
    c_send[...] = count
    c_copies = []
    for d in (2, 1, 3):
        copy = pltpu.make_async_remote_copy(
            src_ref=c_send,
            dst_ref=c_recv.at[d - 1],
            send_sem=c_ssem.at[d - 1],
            recv_sem=c_rsem.at[d - 1],
            device_id={"x": (x + d) % 4},
            device_id_type=MESH,
        )
        copy.start()
        c_copies.append(copy)
    for c in cot_copies:
        c.wait()

    top, low = pl.ds(0, TOP), pl.ds(TOP, F - TOP)
    up, down = (x + 1) % 4, (x + 3) % 4

    def block(to, ref):
        lanes = pl.ds(pl.multiple_of(to * 256, 256), 256)
        acc = jnp.dot(fm[0], cot[0, :, lanes], preferred_element_type=F32)
        for r in range(1, ROWS):
            acc = acc + jnp.dot(fm[r], cot[r, :, lanes], preferred_element_type=F32)
        ref[0] = acc[:, :128]
        ref[1] = acc[:, 128:]

    def x_copy(source, target, sems, i, to):
        return pltpu.make_async_remote_copy(
            src_ref=source,
            dst_ref=target,
            send_sem=sems[0].at[i],
            recv_sem=sems[1].at[i],
            device_id={"x": to},
            device_id_type=MESH,
        )

    ups, downs = (u_ssem, u_rsem), (d_ssem, d_rsem)
    first_up = [x_copy(x_two.at[h, top], s_up.at[h], ups, h, up) for h in range(2)]
    first_down = [x_copy(x_two.at[h, low], s_down.at[h], downs, h, down) for h in range(2)]
    plain_up = [x_copy(x_up.at[h, low], r_up.at[h, low], ups, 2 + h, up) for h in range(2)]
    plain_down = [x_copy(x_down.at[h, top], r_down.at[h, top], downs, 2 + h, down) for h in range(2)]
    sum_up = [x_copy(x_up.at[h, top], r_up.at[h, top], ups, 4 + h, up) for h in range(2)]
    sum_down = [x_copy(x_down.at[h, low], r_down.at[h, low], downs, 4 + h, down) for h in range(2)]

    block((x + 2) % 4, x_two)
    for h in range(2):
        first_up[h].start()
        first_down[h].start()
    block(up, x_up)
    plain_up[0].start()
    block(down, x_down)
    plain_down[0].start()
    block(x, x_own)
    for h in range(2):
        first_up[h].wait_recv()
        x_up[h, top, :] += s_up[h]
        sum_up[h].start()
        first_down[h].wait_recv()
        x_down[h, low, :] += s_down[h]
        sum_down[h].start()
        if h == 0:
            plain_up[1].start()
            plain_down[1].start()
    for copy in c_copies:
        copy.wait_recv()
    counted = c_send[...] + c_recv[0] + c_recv[1] + c_recv[2]
    counted = counted + pltpu.roll(counted, 64, 1)
    half = iota((8, 128), 1) // 64

    def z_copy(to):
        return pltpu.make_async_remote_copy(
            src_ref=z_send.at[to],
            dst_ref=z_recv.at[z],
            send_sem=z_ssem.at[to],
            recv_sem=z_rsem.at[z],
            device_id={"z": to},
            device_id_type=MESH,
        )

    for copy in (plain_up[0], plain_down[0], sum_up[0], sum_down[0]):
        copy.wait_recv()
    def z_half(h):
        total = x_own[h] + r_up[h] + r_down[h]
        turned = jnp.transpose(total[:128, :])
        rest = total[128:F, :]
        for to in ((0, 1), (3, 2))[h]:
            z_send[to, :64, :] = turned[64 * (to % 2) : 64 * (to % 2) + 64, :]
            z_send[to, 64:72, :] = jnp.where(half == to % 2, rest, counted)

            @pl.when(z != to)
            def _():
                z_copy(to).start()

    z_half(0)
    for copy in (plain_up[1], plain_down[1], sum_up[1], sum_down[1]):
        copy.wait_recv()
    z_half(1)

    w_copy.wait()
    for r in range(ROWS):
        v = valid[r][:, :PATCHES]
        v16 = jnp.concatenate([v] * 17, axis=0)
        for p in range(0, PATCHES, 256):
            n = min(256, PATCHES - p)
            product = lax.dot_general(
                w[...], cot[r, p : p + n, :], (((1,), (1,)), ((), ())), preferred_element_type=F32
            )
            fg_ref[r, :, p : p + n] = (product * v16[:, p : p + n]).astype(BF16)

    nearer = z_send[z]
    for d in range(1, 4):
        source = (z + d) % 4
        pltpu.make_async_remote_copy(
            src_ref=z_send.at[source],
            dst_ref=z_recv.at[source],
            send_sem=z_ssem.at[source],
            recv_sem=z_rsem.at[source],
            device_id={"z": source},
            device_id_type=MESH,
        ).wait_recv()
        nearer = nearer + z_recv[source]
    for to in range(8):
        y_send[to, :8, :] = nearer[8 * to : 8 * to + 8, :]
        y_send[to, 8:16, :] = nearer[64:72, :]

    y_copies = []
    for d in (4, 3, 5, 2, 6, 1, 7):
        to = (y + d) % 8
        copy = pltpu.make_async_remote_copy(
            src_ref=y_send.at[to],
            dst_ref=y_recv.at[d - 1],
            send_sem=y_ssem.at[d - 1],
            recv_sem=y_rsem.at[d - 1],
            device_id={"y": to},
            device_id_type=MESH,
        )
        copy.start()
        y_copies.append(copy)
    for copy in y_copies:
        copy.wait_recv()
    last = y_send[y]
    for d in range(7):
        last = last + y_recv[d]
    tile = last[8:16, :]
    other = jnp.where(half == z % 2, 0.0, tile)
    points = jnp.sum(jnp.sum(other, axis=1, keepdims=True), axis=0, keepdims=True)
    scale = lax.rsqrt(jnp.maximum(points, 1.0))
    wg_ref[:, :128] = last[:8, :] * scale
    moved = pltpu.roll(tile, (128 - ((z % 2) * 64 + y * 8)) % 128, 1)
    wg_ref[:, 128:136] = jnp.transpose(moved)[:8, :] * scale

    x_copies = first_up + first_down + plain_up + plain_down + sum_up + sum_down
    for copy in [to_far, to_mate, relay] + x_copies + c_copies + y_copies:
        copy.wait_send()
    for to in range(4):

        @pl.when(z != to)
        def _():
            z_copy(to).wait_send()


def local(field, cotangent, weight, lon_counts, point_mask):
    ft = jnp.transpose(field, (0, 2, 1))
    hbm = pl.BlockSpec(memory_space=pltpu.HBM)
    vmem = pl.BlockSpec(memory_space=pltpu.VMEM)
    dma = pltpu.SemaphoreType.DMA
    fg, wg = pl.pallas_call(
        kernel,
        out_shape=(pltpu.VMEM((ROWS, F, PATCHES), BF16), pltpu.VMEM((8, F), F32)),
        in_specs=[hbm] * 5,
        out_specs=(vmem, vmem),
        scratch_shapes=[
            pltpu.VMEM((ROWS, F, PATCHES), BF16),
            pltpu.VMEM((ROWS, PATCHES, E), BF16),
            pltpu.VMEM((F, E), BF16),
            pltpu.SMEM((ROWS,), jnp.int32),
            pltpu.VMEM((4, ROWS, PART), jnp.int32),
            pltpu.VMEM((4, PART, WIDTH), BF16),
            pltpu.VMEM((ROWS, 8, LANES), F32),
            pltpu.VMEM((ROWS, F, PATCHES), BF16),
            pltpu.VMEM((2, F, 128), F32),
            pltpu.VMEM((2, F, 128), F32),
            pltpu.VMEM((2, F, 128), F32),
            pltpu.VMEM((2, F, 128), F32),
            pltpu.VMEM((2, TOP, 128), F32),
            pltpu.VMEM((2, F - TOP, 128), F32),
            pltpu.VMEM((2, F, 128), F32),
            pltpu.VMEM((2, F, 128), F32),
            pltpu.VMEM((8, 128), F32),
            pltpu.VMEM((3, 8, 128), F32),
            pltpu.VMEM((4, Z_ROWS, 128), F32),
            pltpu.VMEM((4, Z_ROWS, 128), F32),
            pltpu.VMEM((8, 16, 128), F32),
            pltpu.VMEM((7, 16, 128), F32),
            dma((ROWS,)), dma((ROWS,)), dma, dma, dma,
            dma((3,)), dma((3,)), dma((6,)), dma((6,)), dma((6,)), dma((6,)), dma((3,)), dma((3,)),
            dma((4,)), dma((4,)), dma((7,)), dma((7,)),
        ],
        compiler_params=pltpu.CompilerParams(
            collective_id=0, has_side_effects=True, vmem_limit_bytes=40 * 1024 * 1024
        ),
        name="backward",
    )(*(pltpu.with_memory_space_constraint(v, pltpu.HBM) for v in (ft, cotangent, weight, lon_counts, point_mask)))
    return jnp.transpose(fg, (0, 2, 1)), wg


def solution(mesh):
    split = Mesh(mesh.devices.reshape(4, 4, 8, 2, 2), AXES)
    in_specs = (P(LAT, None, CHAN), P(LAT, None, None), P(CHAN, None), P(LAT), P(LAT, CHAN))
    out_specs = (P(LAT, None, CHAN), P(LAT, CHAN))
    return jax.shard_map(local, mesh=split, in_specs=in_specs, out_specs=out_specs, check_vma=False)
```

```python
import functools

import jax
import jax.numpy as jnp
from jax import lax
from jax.experimental import pallas as pl
from jax.experimental.pallas import tpu as pltpu
from jax.sharding import Mesh
from jax.sharding import PartitionSpec as P

MESH = pl.DeviceIdType.MESH
AXES = ("x", "z", "y", "zh", "core")
LAT = ("x", "z", "y")
CHAN = ("zh", "core")
F32 = jnp.float32
BF16 = jnp.bfloat16

ROWS = 5
PATCHES = 642
F = 136
E = 1024
PART = 1284
WIDTH = 384
LANES = 768
Z_ROWS = 9
Y_ROWS = 18
TOP = 72


def iota(shape, dim):
    return lax.broadcasted_iota(jnp.int32, shape, dim)


def kernel(
    ft_hbm, cot_hbm, w_hbm, counts_hbm, mask_hbm,
    fg_ref, wg_ref,
    ft, cot, w, counts, masks, pick, valid, fm,
    x_all, x_own, s_up, s_down, r_all, c_send, c_recv, z_send, z_recv, y_send, y_recv,
    cot_sem, ft_sem, w_sem, counts_sem, mask_sem,
    m_ssem, m_rsem, x_ssem, x_rsem, c_ssem, c_rsem, z_ssem, z_rsem, y_ssem, y_rsem, heard,
):
    x, z, y = (lax.axis_index(a) for a in LAT)
    zh, core = (lax.axis_index(a) for a in CHAN)
    me = zh * 2 + core
    mate = zh * 2 + 1 - core
    far = (1 - zh) * 2 + core
    far_mate = (1 - zh) * 2 + 1 - core

    own_mask = pltpu.make_async_copy(mask_hbm, masks.at[me], mask_sem)
    own_mask.start()
    own_counts = pltpu.make_async_copy(counts_hbm, counts, counts_sem)
    own_counts.start()

    barrier = pltpu.get_barrier_semaphore()

    def greet(device):
        pl.semaphore_signal(barrier, inc=1, device_id=device, device_id_type=MESH)

    def neighbours(signal, axes):
        for axis, at, size in axes:
            signal({axis: (at + 1) % size})
            signal({axis: (at + size - 1) % size})

        @pl.when(z > 0)
        def _():
            signal({"z": z - 1})

        @pl.when(z < 3)
        def _():
            signal({"z": z + 1})

    beside = (z + 3) // 4 + (6 - z) // 4
    greet({"zh": 1 - zh})
    greet({"core": 1 - core})
    neighbours(greet, (("x", x, 4), ("y", y, 8)))

    def hear(i):
        def tell(device):
            pl.semaphore_signal(heard.at[i], inc=1, device_id=device, device_id_type=MESH)

        if i < 2:
            neighbours(tell, (("x", x, 4), ("y", y, 8))[1 - (i == 0) :])
        else:
            tell({"y": (y + 1) % 8})
            tell({"y": (y + 7) % 8})

    shards = (me, mate, far, far_mate)

    def fill(i):
        at = ((iota((PART, WIDTH), 0) + PART * shards[i]) >> 3) - 128 * shards[i]
        hit = at == iota((PART, WIDTH), 1)
        pick[i] = jnp.where(hit, 1.0, 0.0).astype(BF16)

    for i in range(4):
        fill(i)
    valid[...] = jnp.zeros_like(valid)

    own_mask.wait()
    own_counts.wait()
    w_copy = pltpu.make_async_copy(w_hbm, w, w_sem)
    cot_copies = [pltpu.make_async_copy(cot_hbm, cot, cot_sem)]
    ft_copies = [pltpu.make_async_copy(ft_hbm, ft, ft_sem)]

    def mask_to(i, shard, device):
        return pltpu.make_async_remote_copy(
            src_ref=masks.at[shard],
            dst_ref=masks.at[shard],
            send_sem=m_ssem,
            recv_sem=m_rsem.at[i],
            device_id=device,
            device_id_type=MESH,
        )

    def place(i):
        j = shards[i]
        spot = iota((8, PART), 1) + PART * j
        phase = (spot & 7) == iota((8, PART), 0)
        rows = []
        for r in range(ROWS):
            keep = jnp.logical_and(phase, spot < counts[r])
            line = jnp.broadcast_to(masks[j, r : r + 1, :], (8, PART)).astype(F32)
            rows.append(jnp.where(keep, line, 0.0))
        spread = jnp.concatenate(rows, axis=0).astype(BF16)
        placed = jnp.dot(spread, pick[i], preferred_element_type=F32)
        lanes = pl.ds(pl.multiple_of(j * 128, 128), WIDTH)
        for r in range(ROWS):
            valid[r, :, lanes] += placed[8 * r : 8 * r + 8]

    for c in ft_copies + cot_copies + [w_copy]:
        c.start()
    pl.semaphore_wait(barrier, 6 + beside)
    to_far = mask_to(0, me, {"zh": 1 - zh})
    to_far.start()
    to_mate = mask_to(1, me, {"core": 1 - core})
    to_mate.start()
    hear(0)
    place(0)
    to_mate.wait_recv()
    place(1)
    to_far.wait_recv()
    relay = mask_to(2, far, {"core": 1 - core})
    relay.start()
    place(2)
    for c in ft_copies:
        c.wait()
    relay.wait_recv()
    place(3)

    count = jnp.zeros((8, 128), F32)
    for r in range(ROWS):
        v = valid[r]
        for t in range(LANES // 128):
            count = count + v[:, 128 * t : 128 * t + 128]
        v = v[:, :PATCHES]
        v16 = jnp.concatenate([v, v], axis=0).astype(BF16)
        for c in range(0, 128, 16):
            fm[r, c : c + 16, :] = ft[r, c : c + 16, :] * v16
        fm[r, 128:136, :] = ft[r, 128:136, :] * v16[:8]
    c_send[...] = count
    for c in cot_copies:
        c.wait()

    top, low = pl.ds(0, TOP), pl.ds(TOP, F - TOP)
    up, down = (x + 1) % 4, (x + 3) % 4

    def block(to, ref):
        lanes = pl.ds(pl.multiple_of(to * 256, 256), 256)
        acc = jnp.dot(fm[0], cot[0, :, lanes], preferred_element_type=F32)
        for r in range(1, ROWS):
            acc = acc + jnp.dot(fm[r], cot[r, :, lanes], preferred_element_type=F32)
        ref[0] = acc[:, :128]
        ref[1] = acc[:, 128:]

    def x_copy(source, target, sem, to):
        return pltpu.make_async_remote_copy(
            src_ref=source,
            dst_ref=target,
            send_sem=x_ssem,
            recv_sem=sem,
            device_id={"x": to},
            device_id_type=MESH,
        )

    def joint(source, target, ssem, rsem, device):
        return pltpu.make_async_remote_copy(
            src_ref=source, dst_ref=target, send_sem=ssem, recv_sem=rsem, device_id=device, device_id_type=MESH
        )

    x_two, x_up, x_down = (x_all.at[i] for i in range(3))
    both = range(2)
    first_up = [x_copy(x_all.at[0, h, top], s_up.at[h], x_rsem.at[h], up) for h in both]
    first_down = [x_copy(x_all.at[0, h, low], s_down.at[h], x_rsem.at[2 + h], down) for h in both]
    plain_up = [x_copy(x_all.at[1, h, low], r_all.at[h, 0, low], x_rsem.at[4 + h], up) for h in both]
    plain_down = [x_copy(x_all.at[2, h, top], r_all.at[h, 1, top], x_rsem.at[4 + h], down) for h in both]
    sum_up = [x_copy(x_all.at[1, h, top], r_all.at[h, 0, top], x_rsem.at[4 + h], up) for h in both]
    sum_down = [x_copy(x_all.at[2, h, low], r_all.at[h, 1, low], x_rsem.at[4 + h], down) for h in both]
    x_in = [x_copy(r_all.at[h], r_all.at[h], x_rsem.at[4 + h], up) for h in both]

    block((x + 2) % 4, x_two)
    for h in range(2):
        first_up[h].start()
        first_down[h].start()
    pl.semaphore_wait(heard.at[0], 4 + beside)
    hear(1)
    for d in (2, 1, 3):
        copy = pltpu.make_async_remote_copy(
            src_ref=c_send,
            dst_ref=c_recv.at[d - 1],
            send_sem=c_ssem,
            recv_sem=c_rsem,
            device_id={"x": (x + d) % 4},
            device_id_type=MESH,
        )
        copy.start()
    block(up, x_up)
    plain_up[0].start()
    block(down, x_down)
    plain_down[0].start()
    block(x, x_own)
    pl.semaphore_wait(heard.at[1], 2 + beside)
    hear(2)
    for h in range(2):
        first_up[h].wait_recv()
        x_up[h, top, :] += s_up[h]
        sum_up[h].start()
        first_down[h].wait_recv()
        x_down[h, low, :] += s_down[h]
        sum_down[h].start()
        if h == 0:
            plain_up[1].start()
            plain_down[1].start()
    joint(c_recv, c_recv, c_ssem, c_rsem, {"x": up}).wait_recv()
    counted = c_send[...] + c_recv[0] + c_recv[1] + c_recv[2]
    counted = jnp.sum(counted, axis=0, keepdims=True)
    counted = counted + pltpu.roll(counted, 64, 1)
    half = iota((1, 128), 1) // 64

    def y_copy(h, d):
        to = (y + d) % 8
        return pltpu.make_async_remote_copy(
            src_ref=y_send.at[h, to],
            dst_ref=y_recv.at[h, d - 1],
            send_sem=y_ssem,
            recv_sem=y_rsem.at[h],
            device_id={"y": to},
            device_id_type=MESH,
        )

    def z_copy(to):
        return pltpu.make_async_remote_copy(
            src_ref=z_send.at[to],
            dst_ref=z_recv.at[(z - to + 3) % 4],
            send_sem=z_ssem,
            recv_sem=z_rsem,
            device_id={"z": to},
            device_id_type=MESH,
        )

    def y_half(h):
        total = x_own[h] + r_all[h, 0] + r_all[h, 1]
        turned = jnp.transpose(total[:128, :])
        rest = jnp.transpose(jnp.concatenate([total[128:F, :], jnp.zeros((120, 128), F32)], axis=0))
        for to in range(8):
            lines = jnp.zeros((8, 128), F32)
            for i in range(2):
                at = 64 * i + 8 * to
                y_send[h, to, 8 * i : 8 * i + 8, :] = turned[at : at + 8, :]
                lines = lines + pltpu.roll(rest[at : at + 8, :], 64 * i, 1, stride=8, stride_axis=0)
            y_send[h, to, 16:17, :] = jnp.sum(lines, axis=0, keepdims=True)
            y_send[h, to, 17:18, :] = counted
        for d in (4, 3, 5, 2, 6, 1, 7):
            y_copy(h, d).start()

    def z_half(h):
        joint(y_recv.at[h], y_recv.at[h], y_ssem, y_rsem.at[h], {"y": (y + 1) % 8}).wait_recv()
        near = y_send[h, y]
        for d in range(7):
            near = near + y_recv[h, d]
        for i in range(2):
            to = 2 * h + (i if h == 0 else 1 - i)
            z_send[to, :8, :] = near[8 * (to % 2) : 8 * (to % 2) + 8, :]
            z_send[to, 8:9, :] = jnp.where(half == to % 2, near[16:17, :], near[17:18, :])

            @pl.when(z != to)
            def _():
                z_copy(to).start()

    x_in[0].wait_recv()
    pl.semaphore_wait(heard.at[2], 2)
    y_half(0)
    x_in[1].wait_recv()
    y_half(1)

    w_copy.wait()
    for r in range(ROWS):
        v = valid[r][:, :PATCHES]
        v16 = jnp.concatenate([v] * 17, axis=0)
        for p in range(0, PATCHES, 256):
            n = min(256, PATCHES - p)
            product = lax.dot_general(
                w[...], cot[r, p : p + n, :], (((1,), (1,)), ((), ())), preferred_element_type=F32
            )
            fg_ref[r, :, p : p + n] = (product * v16[:, p : p + n]).astype(BF16)

    z_half(0)
    z_half(1)
    joint(z_recv, z_recv, z_ssem, z_rsem, {"z": (z + 1) % 4}).wait_recv()
    last = z_send[z] + z_recv[0] + z_recv[1] + z_recv[2]
    row = last[8:9, :]
    mine = half == z % 2
    points = jnp.sum(jnp.where(mine, 0.0, row), axis=1, keepdims=True)
    scale = lax.rsqrt(jnp.maximum(points, 1.0))
    wg_ref[:, :128] = last[:8, :] * scale
    kept = jnp.logical_and(((iota((8, 128), 1) >> 3) & 7) == iota((8, 128), 0), iota((8, 128), 1) // 64 == z % 2)
    tail = jnp.where(kept, jnp.broadcast_to(row, (8, 128)), 0.0)
    for step in (64, 32, 16, 8):
        tail = tail + pltpu.roll(tail, step, 1)
    wg_ref[:, 128:136] = tail[:, :8] * scale

    mask_to(0, pl.ds(0, 3), {"zh": 1 - zh}).wait_send()
    x_copy(x_all, x_all, x_rsem.at[0], up).wait_send()
    joint(c_recv, c_recv, c_ssem, c_rsem, {"x": up}).wait_send()
    joint(z_recv, z_recv, z_ssem, z_rsem, {"z": (z + 1) % 4}).wait_send()
    joint(y_recv, y_recv, y_ssem, y_rsem.at[0], {"y": (y + 1) % 8}).wait_send()


def store(fg, wg, fg_hbm, wg_hbm, fg_sem, wg_sem):
    copies = [pltpu.make_async_copy(wg, wg_hbm, wg_sem), pltpu.make_async_copy(fg, fg_hbm, fg_sem)]
    for copy in copies:
        copy.start()
    for copy in copies:
        copy.wait()


def local(field, cotangent, weight, lon_counts, point_mask):
    ft = jnp.transpose(field, (0, 2, 1))
    hbm = pl.BlockSpec(memory_space=pltpu.HBM)
    vmem = pl.BlockSpec(memory_space=pltpu.VMEM)
    dma = pltpu.SemaphoreType.DMA
    fg, wg = pl.pallas_call(
        kernel,
        out_shape=(pltpu.VMEM((ROWS, F, PATCHES), BF16), pltpu.VMEM((8, F), F32)),
        in_specs=[hbm] * 5,
        out_specs=(vmem, vmem),
        scratch_shapes=[
            pltpu.VMEM((ROWS, F, PATCHES), BF16),
            pltpu.VMEM((ROWS, PATCHES, E), BF16),
            pltpu.VMEM((F, E), BF16),
            pltpu.SMEM((ROWS,), jnp.int32),
            pltpu.VMEM((4, ROWS, PART), jnp.int32),
            pltpu.VMEM((4, PART, WIDTH), BF16),
            pltpu.VMEM((ROWS, 8, LANES), F32),
            pltpu.VMEM((ROWS, F, PATCHES), BF16),
            pltpu.VMEM((3, 2, F, 128), F32),
            pltpu.VMEM((2, F, 128), F32),
            pltpu.VMEM((2, TOP, 128), F32),
            pltpu.VMEM((2, F - TOP, 128), F32),
            pltpu.VMEM((2, 2, F, 128), F32),
            pltpu.VMEM((8, 128), F32),
            pltpu.VMEM((3, 8, 128), F32),
            pltpu.VMEM((4, Z_ROWS, 128), F32),
            pltpu.VMEM((3, Z_ROWS, 128), F32),
            pltpu.VMEM((2, 8, Y_ROWS, 128), F32),
            pltpu.VMEM((2, 7, Y_ROWS, 128), F32),
            dma, dma, dma, dma, dma,
            dma, dma((3,)), dma, dma((6,)), dma, dma, dma, dma, dma, dma((2,)),
            pltpu.SemaphoreType.REGULAR((3,)),
        ],
        compiler_params=pltpu.CompilerParams(
            collective_id=0, has_side_effects=True, vmem_limit_bytes=40 * 1024 * 1024
        ),
        name="backward",
    )(*(pltpu.with_memory_space_constraint(v, pltpu.HBM) for v in (ft, cotangent, weight, lon_counts, point_mask)))
    fg, wg = pl.pallas_call(
        store,
        out_shape=(
            jax.ShapeDtypeStruct((ROWS, F, PATCHES), BF16),
            jax.ShapeDtypeStruct((8, F), F32),
        ),
        in_specs=[vmem] * 2,
        out_specs=(hbm, hbm),
        scratch_shapes=[dma, dma],
        name="store",
    )(*(pltpu.with_memory_space_constraint(v, pltpu.VMEM) for v in (fg, wg)))
    return jnp.transpose(fg, (0, 2, 1)), wg


def solution(mesh):
    split = Mesh(mesh.devices.reshape(4, 4, 8, 2, 2), AXES)
    in_specs = (P(LAT, None, CHAN), P(LAT, None, None), P(CHAN, None), P(LAT), P(LAT, CHAN))
    out_specs = (P(LAT, None, CHAN), P(LAT, CHAN))
    return jax.shard_map(local, mesh=split, in_specs=in_specs, out_specs=out_specs, check_vma=False)
```
